32 devices in a mesh: layer: 2 (over x), blk: 16 (over z, y, core).
Axes of the slice: x: 2, y: 2, z: 4, core: 2. Of those that a mesh axis runs over, the one named last changes fastest.
Arguments:
- points: bfloat16 [12288, 256], P('blk'), may hold values from -8.4 to 8.4
- labels: int32 [12288], P('blk'), may hold values from 0 to 255, as said below
Outputs:
- distance: float32 [12288, 256], P('blk')
The draws below stay inside these ranges and needn't reach their ends.
Inputs may be any that keep to these rules, and one draw needn't show every extreme that they name: `labels`: every cluster is named by at least one point.
All inputs are finite; a program needn't handle non-finite values.
Results may differ from the reference program's by a relative error of at most 0.00034.
Values may be sent and summed in bfloat16 or wider, within the bound.
A program may use at most 64 MiB of HBM per device.

```python
import jax
import jax.numpy as jnp
from jax import lax

D = 256
K = 256
P_DEV = 768
NPOINTS = 12288


def make_labels(key):
    point_index = jnp.arange(NPOINTS, dtype=jnp.int32)
    home_slot = point_index * K // NPOINTS
    near_step = jax.random.randint(jax.random.fold_in(key, 1), (NPOINTS,), -2, 3)
    spread = jax.random.randint(jax.random.fold_in(key, 2), (NPOINTS,), 0, K)
    coin_flip = jax.random.randint(jax.random.fold_in(key, 3), (NPOINTS,), 0, 4)
    labelled = jnp.where(coin_flip < 3, (home_slot + near_step) % K, spread)
    ordering = jax.random.permutation(jax.random.fold_in(key, 4), NPOINTS)
    labelled = labelled.at[ordering[:K]].set(jnp.arange(K, dtype=jnp.int32))
    return labelled.astype(jnp.int32)


def draw_labels(key, part):
    return make_labels(jax.random.fold_in(key, 11))


def draw_points(key, part):
    labelled = make_labels(jax.random.fold_in(key, 11))
    centers = jnp.clip(jax.random.normal(jax.random.fold_in(key, 12), (K, D), jnp.float32), -4.0, 4.0)
    noise_part = jnp.clip(jax.random.normal(jax.random.fold_in(key, 13), (NPOINTS, D), jnp.float32), -4.0, 4.0)
    based = 0.6 * centers[labelled] + 0.8 * noise_part
    log_scale = jax.random.uniform(jax.random.fold_in(key, 14), (NPOINTS,), jnp.float32, jnp.log(0.15), jnp.log(1.5))
    row_scale = jnp.exp(log_scale)
    return (row_scale[:, None] * based).astype(jnp.bfloat16)


def setup_inputs(seed: int = 0) -> dict:
    arg_keys = jax.random.split(jax.random.key(seed), 3)
    return {
        "points": draw_points(jax.random.fold_in(arg_keys[2], 71), 0),
        "labels": draw_labels(jax.random.fold_in(arg_keys[2], 71), 0),
    }


def reference(points, labels):
    point_count = points.shape[0]
    point_sq = jnp.sum(jnp.square(points.astype(jnp.float32)), axis=1)
    member = (labels[:, None] == jnp.arange(K, dtype=jnp.int32)[None, :]).astype(jnp.bfloat16)

    def one_block(first_row):
        row_block = lax.dynamic_slice_in_dim(points, first_row, P_DEV, 0)
        row_sq = lax.dynamic_slice_in_dim(point_sq, first_row, P_DEV, 0)
        gram_block = lax.dot_general(row_block, points, (((1,), (1,)), ((), ())), preferred_element_type=jnp.float32)
        kernel = jnp.exp(-(row_sq[:, None] + point_sq[None, :] - 2.0 * gram_block) / D).astype(jnp.bfloat16)
        return jnp.dot(kernel, member, preferred_element_type=jnp.float32)

    starts = (jnp.arange(point_count // P_DEV, dtype=jnp.int32) * P_DEV).astype(jnp.int32)
    row_sums = lax.map(one_block, starts).reshape(point_count, K)
    member_f = member.astype(jnp.float32)
    counts = jnp.sum(member_f, axis=0)
    within = jnp.sum(member_f * row_sums, axis=0)
    return 1.0 - 2.0 * row_sums / counts[None, :] + within[None, :] / (counts * counts)[None, :]
```

```python
import functools
import math

import jax
import jax.numpy as jnp
from jax import lax
from jax.experimental import pallas as pl
from jax.experimental.pallas import tpu as pltpu
from jax.sharding import PartitionSpec as P

K = 256
MESH = pl.DeviceIdType.MESH
NT = (((1,), (1,)), ((), ()))
CW, CCW = 0, 1
AUX, TX = 2, 3


def kernel(layers, nb, p_ref, lab_ref, out_ref, buf, aux, acc, mem_acc, rcol, lcol, own_aux, wsrc, wbuf,
           local_sem, ring_s, ring_r, d2d_s, d2d_r, x_s, x_r, w_s, w_r):
    rows, feat = p_ref.shape
    third = rows // 3
    groups = nb // 2
    far = groups // 2
    layer = lax.axis_index("layer")
    me = lax.axis_index("blk")
    core = me % 2
    group = me // 2
    low, odd = group // 2, group % 2
    place = low + odd * (groups - 1 - 2 * low)

    def group_at(pos):
        pos = (pos + groups) % groups
        side = pos // far
        return 2 * (pos + side * (groups - 1 - 2 * pos)) + side

    other_layer = layer + 1 - 2 * (layer % 2)
    side = layer % 2
    partner = 2 * group + 1 - core
    nexts = (2 * group_at(place + 1) + core, 2 * group_at(place - 1) + core)
    piece_x, piece_tx = 2 * side, 2 - 2 * side

    def from_at(way, d):
        return group_at(place - d) if way == CW else group_at(place + d)

    def ring_copy(src, way, d, item, device=None):
        return pltpu.make_async_remote_copy(
            src_ref=src, dst_ref=src, send_sem=ring_s.at[way, d, item], recv_sem=ring_r.at[way, d, item],
            device_id=(layer, nexts[way]), device_id_type=MESH)

    def d2d_copy(src, way, d, item):
        return pltpu.make_async_remote_copy(
            src_ref=src, dst_ref=src, send_sem=d2d_s.at[way, d, item], recv_sem=d2d_r.at[way, d, item],
            device_id=(layer, partner), device_id_type=MESH)

    def x_copy(src, way, d):
        return pltpu.make_async_remote_copy(
            src_ref=src, dst_ref=src, send_sem=x_s.at[way, d], recv_sem=x_r.at[way, d],
            device_id=(other_layer, me), device_id_type=MESH)

    own_load = [pltpu.make_async_copy(p_ref.at[pl.ds(t * third, third)], buf.at[me, t], local_sem.at[t])
                for t in range(3)]
    for copy in own_load:
        copy.start()

    barrier = pltpu.get_barrier_semaphore()

    def greet(o, carry):
        pl.semaphore_signal(barrier, inc=1, device_id=(layer, (me + o) % nb), device_id_type=MESH)
        return carry

    lax.fori_loop(1, nb, greet, 0)
    pl.semaphore_signal(barrier, inc=1, device_id=(other_layer, me), device_id_type=MESH)
    for copy in own_load:
        copy.wait()

    scale = math.log2(math.e) / feat
    for t in range(3):
        part = slice(t * third, (t + 1) * third)
        x = buf[me, t].astype(jnp.float32)
        sq = jnp.sum(x * x, axis=1, keepdims=True) * scale
        wide = jnp.broadcast_to(sq, (third, 128))
        rcol[part, :] = wide
        own_aux[:, part] = wide.T[0:1, :]
    lab = lab_ref[...].astype(jnp.float32)
    own_aux[:, rows:] = lab
    lcol[...] = jnp.broadcast_to(lab, (128, rows)).T
    acc[...] = jnp.zeros_like(acc)
    mem_acc[...] = jnp.zeros_like(mem_acc)
    pl.semaphore_wait(barrier, nb)

    def aux_send(way):
        return pltpu.make_async_remote_copy(
            src_ref=own_aux, dst_ref=aux.at[me], send_sem=ring_s.at[way, 1, AUX], recv_sem=ring_r.at[way, 1, AUX],
            device_id=(layer, nexts[way]), device_id_type=MESH)

    aux_d2d = pltpu.make_async_remote_copy(
        src_ref=own_aux, dst_ref=aux.at[me], send_sem=d2d_s.at[CW, 0, AUX], recv_sem=d2d_r.at[CW, 0, AUX],
        device_id=(layer, partner), device_id_type=MESH)

    for way in (CW, CCW):
        aux_send(way).start()
    ring_copy(buf.at[me, piece_x], CW, 1, 0).start()
    ring_copy(buf.at[me, 1], CCW, 1, 0).start()
    ring_copy(buf.at[me, 1], CW, 1, 1).start()
    ring_copy(buf.at[me, piece_x], CCW, 1, 1).start()
    aux_d2d.start()
    d2d_copy(buf.at[me], CW, 0, 0).start()

    ids = lax.broadcasted_iota(jnp.int32, (K, third), 0).astype(jnp.float32)
    own_copy = pltpu.make_async_copy(own_aux, aux.at[me], local_sem.at[0])
    own_copy.start()
    own_copy.wait()

    def visit(b, piece, offset):
        cols = buf[b, piece]
        col_sq = aux[b, :, pl.ds(offset, third)]
        tags = aux[b, :, pl.ds(pl.multiple_of(rows + offset, 128), third)]
        member = (tags == ids).astype(jnp.float32)
        mem_acc[...] += member
        member = member.astype(jnp.bfloat16)
        for r in range(3):
            part = slice(r * third, (r + 1) * third)
            gram = lax.dot_general(buf[me, r], cols, NT, preferred_element_type=jnp.float32)
            row_sq = rcol[part, :]
            row_sq = jnp.concatenate([row_sq] * (third // 128), axis=1)
            kern = jnp.exp2(gram * (2.0 * scale) - (row_sq + col_sq)).astype(jnp.bfloat16)
            acc[part, :] += lax.dot_general(kern, member, NT, preferred_element_type=jnp.float32)

    def see(b, piece):
        visit(b, piece, pl.multiple_of(piece * third, 128))

    def see_all(b):
        def one(t, carry):
            see(b, t)
            return carry
        lax.fori_loop(0, 3, one, 0)

    see_all(me)
    aux_d2d.wait_recv()
    d2d_copy(buf.at[partner], CW, 0, 0).wait_recv()
    see_all(partner)

    def ring_arrival(way, d, item, piece, onward, to_x):
        b = 2 * from_at(way, d) + core
        ref = buf.at[b, piece]
        ring_copy(ref, way, d, item).wait_recv()
        if onward:
            ring_copy(ref, way, d + 1, item).start()
        if to_x:
            x_copy(ref, way, d).start()
        d2d_copy(ref, way, d, item).start()

    def aux_arrival(way, d, onward):
        b = 2 * from_at(way, d) + core
        ref = aux.at[b]
        ring_copy(ref, way, d, AUX).wait_recv()
        if onward:
            ring_copy(ref, way, d + 1, AUX).start()
        d2d_copy(ref, way, d, AUX).start()

    def x_arrival(way, d, onward):
        b = 2 * from_at(way, d) + core
        ref = buf.at[b, piece_tx]
        x_copy(ref, way, d).wait_recv()
        if onward:
            ring_copy(ref, way, d + 1, TX).start()
        d2d_copy(ref, way, d, TX).start()

    def d2d_arrival(way, d, item, piece):
        b = 2 * from_at(way, d) + 1 - core
        ref = aux.at[b] if item == AUX else buf.at[b, piece]
        d2d_copy(ref, way, d, item).wait_recv()

    def see_list(entries):
        for way, d, item, piece in entries:
            see(2 * from_at(way, d) + core, piece)
        for way, d, item, piece in entries:
            d2d_arrival(way, d, item, piece)
            see(2 * from_at(way, d) + 1 - core, piece)

    def turn(d, with_x, last):
        for way in (CW, CCW):
            aux_arrival(way, d, onward=not last or way == CW)
        ring_arrival(CW, d, 0, piece_x, onward=True, to_x=True)
        ring_arrival(CCW, d, 0, 1, onward=True, to_x=False)
        if with_x:
            x_arrival(CW, d - 1, False)
        for way in (CW, CCW):
            d2d_arrival(way, d, AUX, None)
        entries = [(CW, d, 0, piece_x), (CCW, d, 0, 1)]
        if with_x:
            entries.append((CW, d - 1, TX, piece_tx))
        see_list(entries)
        ring_arrival(CW, d, 1, 1, onward=not last, to_x=False)
        ring_arrival(CCW, d, 1, piece_x, onward=not last, to_x=True)
        if with_x:
            x_arrival(CCW, d - 1, False)
        entries = [(CW, d, 1, 1), (CCW, d, 1, piece_x)]
        if with_x:
            entries.append((CCW, d - 1, TX, piece_tx))
        see_list(entries)

    turn(1, False, far == 2)
    if far > 3:
        lax.fori_loop(2, far - 1, lambda d, c: (turn(d, True, False), c)[1], 0)
    if far > 2:
        turn(far - 1, True, True)
    x_arrival(CW, far - 1, True)
    aux_arrival(CW, far, False)
    ring_arrival(CW, far, 0, piece_x, False, False)
    ring_arrival(CCW, far, 0, 1, False, False)
    d2d_arrival(CW, far, AUX, None)
    see_list([(CW, far - 1, TX, piece_tx), (CW, far, 0, piece_x), (CCW, far, 0, 1)])
    x_arrival(CCW, far - 1, False)
    see_list([(CCW, far - 1, TX, piece_tx)])
    ring_arrival(CW, far, TX, piece_tx, False, False)
    see_list([(CW, far, TX, piece_tx)])

    lane = lax.broadcasted_iota(jnp.int32, (rows, 128), 1).astype(jnp.float32)
    for h in range(K // 128):
        cut = slice(h * 128, (h + 1) * 128)
        mine = jnp.where(lcol[...] == lane + float(h * 128), acc[:, cut], 0.0)
        wsrc[:, cut] = jnp.sum(mine, axis=0, keepdims=True)

    def within_copy(o, sender):
        return pltpu.make_async_remote_copy(
            src_ref=wsrc, dst_ref=wbuf.at[sender], send_sem=w_s.at[o], recv_sem=w_r.at[o],
            device_id=(layer, (me + o) % nb), device_id_type=MESH)

    def send_within(o, carry):
        within_copy(o, me).start()
        return carry

    lax.fori_loop(1, nb, send_within, 0)
    ones = jnp.ones((8, K), jnp.bfloat16)
    counts = lax.dot_general(ones, mem_acc[...].astype(jnp.bfloat16).T, (((1,), (0,)), ((), ())),
                             preferred_element_type=jnp.float32)[0:1, :]
    factor = 2.0 / counts
    acc[...] = 1.0 - acc[...] * factor

    def drain(d):
        for way in (CW, CCW):
            for item in (0, 1):
                ring_copy(buf.at[me, 0], way, d, item).wait_send()
                d2d_copy(buf.at[me, 0], way, d, item).wait_send()
            ring_copy(aux.at[me], way, d, AUX).wait_send()
            d2d_copy(aux.at[me], way, d, AUX).wait_send()
            d2d_copy(buf.at[me, 0], way, d, TX).wait_send()
            x_copy(buf.at[me, 0], way, d).wait_send()

    lax.fori_loop(1, far, lambda d, c: (drain(d), c)[1], 0)
    ring_copy(buf.at[me, 0], CW, far, 0).wait_send()
    ring_copy(buf.at[me, 0], CCW, far, 0).wait_send()
    ring_copy(buf.at[me, 0], CW, far, TX).wait_send()
    ring_copy(aux.at[me], CW, far, AUX).wait_send()
    d2d_copy(buf.at[me, 0], CW, far, 0).wait_send()
    d2d_copy(buf.at[me, 0], CCW, far, 0).wait_send()
    d2d_copy(buf.at[me, 0], CW, far, TX).wait_send()
    d2d_copy(aux.at[me], CW, far, AUX).wait_send()
    d2d_copy(aux.at[me], CW, 0, AUX).wait_send()
    d2d_copy(buf.at[me], CW, 0, 0).wait_send()

    def wait_within(o, total):
        sender = (me - o + nb) % nb
        copy = within_copy(o, sender)
        copy.wait_recv()
        copy.wait_send()
        return total + wbuf[sender]

    within = lax.fori_loop(1, nb, wait_within, wsrc[...])
    out_ref[...] = acc[...] + within / (counts * counts)


def solution(mesh):
    layers, nb = mesh.shape["layer"], mesh.shape["blk"]

    def shards(points, labels):
        rows, feat = points.shape
        third = rows // 3
        far = nb // 4
        sems = pltpu.SemaphoreType.DMA
        return pl.pallas_call(
            functools.partial(kernel, layers, nb),
            out_shape=jax.ShapeDtypeStruct((rows, K), jnp.float32),
            in_specs=[pl.BlockSpec(memory_space=pl.ANY), pl.BlockSpec(memory_space=pltpu.VMEM)],
            out_specs=pl.BlockSpec(memory_space=pltpu.VMEM),
            scratch_shapes=[
                pltpu.VMEM((nb, 3, third, feat), jnp.bfloat16),
                pltpu.VMEM((nb, 1, 2 * rows), jnp.float32),
                pltpu.VMEM((rows, K), jnp.float32),
                pltpu.VMEM((K, third), jnp.float32),
                pltpu.VMEM((rows, 128), jnp.float32),
                pltpu.VMEM((rows, 128), jnp.float32),
                pltpu.VMEM((1, 2 * rows), jnp.float32),
                pltpu.VMEM((1, K), jnp.float32),
                pltpu.VMEM((nb, 1, K), jnp.float32),
                sems((3,)),
                sems((2, far + 1, 4)),
                sems((2, far + 1, 4)),
                sems((2, far + 1, 4)),
                sems((2, far + 1, 4)),
                sems((2, far + 1)),
                sems((2, far + 1)),
                sems((nb,)),
                sems((nb,)),
            ],
            compiler_params=pltpu.CompilerParams(
                collective_id=0, has_side_effects=True, vmem_limit_bytes=60 * 1024 * 1024),
        )(points, labels.reshape(1, rows))

    return jax.shard_map(
        shards, mesh=mesh, in_specs=(P("blk", None), P("blk")), out_specs=P("blk", None), check_vma=False)
```

```python
import functools
import math

import jax
import jax.numpy as jnp
from jax import lax
from jax.experimental import pallas as pl
from jax.experimental.pallas import tpu as pltpu
from jax.sharding import PartitionSpec as P

K = 256
MESH = pl.DeviceIdType.MESH
NT = (((1,), (1,)), ((), ()))
CW, CCW = 0, 1
AUX, TX = 2, 3


def kernel(layers, nb, p_ref, lab_ref, out_ref, buf, aux, acc, mem_acc, rcol, lcol, own_aux, wsrc, wbuf,
           local_sem, ring_s, ring_r, d2d_s, d2d_r, x_s, x_r, w_s, w_r):
    rows, feat = p_ref.shape
    third = rows // 3
    groups = nb // 2
    far = groups // 2
    layer = lax.axis_index("layer")
    me = lax.axis_index("blk")
    core = me % 2
    group = me // 2
    low, odd = group // 2, group % 2
    place = low + odd * (groups - 1 - 2 * low)

    def group_at(pos):
        pos = (pos + groups) % groups
        side = pos // far
        return 2 * (pos + side * (groups - 1 - 2 * pos)) + side

    other_layer = layer + 1 - 2 * (layer % 2)
    side = layer % 2
    partner = 2 * group + 1 - core
    nexts = (2 * group_at(place + 1) + core, 2 * group_at(place - 1) + core)
    piece_x, piece_tx = 2 * side, 2 - 2 * side

    def from_at(way, d):
        return group_at(place - d) if way == CW else group_at(place + d)

    def ring_copy(src, way, d, item, device=None):
        return pltpu.make_async_remote_copy(
            src_ref=src, dst_ref=src, send_sem=ring_s.at[way, d, item], recv_sem=ring_r.at[way, d, item],
            device_id=(layer, nexts[way]), device_id_type=MESH)

    def d2d_copy(src, way, d, item):
        return pltpu.make_async_remote_copy(
            src_ref=src, dst_ref=src, send_sem=d2d_s.at[way, d, item], recv_sem=d2d_r.at[way, d, item],
            device_id=(layer, partner), device_id_type=MESH)

    def x_copy(src, way, d):
        return pltpu.make_async_remote_copy(
            src_ref=src, dst_ref=src, send_sem=x_s.at[way, d], recv_sem=x_r.at[way, d],
            device_id=(other_layer, me), device_id_type=MESH)

    own_load = [pltpu.make_async_copy(p_ref.at[pl.ds(t * third, third)], buf.at[me, t], local_sem.at[t])
                for t in range(3)]
    for copy in own_load:
        copy.start()

    barrier = pltpu.get_barrier_semaphore()

    for place_of in ((layer, nexts[CW]), (layer, nexts[CCW]), (layer, partner), (other_layer, me)):
        pl.semaphore_signal(barrier, inc=1, device_id=place_of, device_id_type=MESH)
    for copy in own_load:
        copy.wait()

    pl.semaphore_wait(barrier, 4)
    ring_copy(buf.at[me, piece_x], CW, 1, 0).start()
    ring_copy(buf.at[me, 1], CCW, 1, 0).start()
    d2d_copy(buf.at[me], CW, 0, 0).start()

    scale = math.log2(math.e) / feat
    for t in range(3):
        part = slice(t * third, (t + 1) * third)
        x = buf[me, t].astype(jnp.float32)
        sq = jnp.sum(x * x, axis=1, keepdims=True) * scale
        wide = jnp.broadcast_to(sq, (third, 128))
        rcol[part, :] = wide
        own_aux[:, part] = wide.T[0:1, :]
    lab = lab_ref[...].reshape(1, rows).astype(jnp.float32)
    own_aux[:, rows:] = lab
    lcol[...] = jnp.broadcast_to(lab, (128, rows)).T
    acc[...] = jnp.zeros_like(acc)
    mem_acc[...] = jnp.zeros_like(mem_acc)

    def aux_send(way):
        return pltpu.make_async_remote_copy(
            src_ref=own_aux, dst_ref=aux.at[me], send_sem=ring_s.at[way, 1, AUX], recv_sem=ring_r.at[way, 1, AUX],
            device_id=(layer, nexts[way]), device_id_type=MESH)

    aux_d2d = pltpu.make_async_remote_copy(
        src_ref=own_aux, dst_ref=aux.at[me], send_sem=d2d_s.at[CW, 0, AUX], recv_sem=d2d_r.at[CW, 0, AUX],
        device_id=(layer, partner), device_id_type=MESH)

    for way in (CW, CCW):
        aux_send(way).start()
    ring_copy(buf.at[me, 1], CW, 1, 1).start()
    ring_copy(buf.at[me, piece_x], CCW, 1, 1).start()
    aux_d2d.start()

    ids = lax.broadcasted_iota(jnp.int32, (K, third), 0).astype(jnp.float32)
    own_copy = pltpu.make_async_copy(own_aux, aux.at[me], local_sem.at[0])
    own_copy.start()
    own_copy.wait()

    def visit(b, piece, offset):
        cols = buf[b, piece]
        col_sq = aux[b, :, pl.ds(offset, third)]
        tags = aux[b, :, pl.ds(pl.multiple_of(rows + offset, 128), third)]
        member = (tags == ids).astype(jnp.float32)
        mem_acc[...] += member
        member = member.astype(jnp.bfloat16)
        for r in range(3):
            part = slice(r * third, (r + 1) * third)
            gram = lax.dot_general(buf[me, r], cols, NT, preferred_element_type=jnp.float32)
            row_sq = rcol[part, :]
            row_sq = jnp.concatenate([row_sq] * (third // 128), axis=1)
            kern = jnp.exp2(gram * (2.0 * scale) - (row_sq + col_sq)).astype(jnp.bfloat16)
            acc[part, :] += lax.dot_general(kern, member, NT, preferred_element_type=jnp.float32)

    def see(b, piece):
        visit(b, piece, pl.multiple_of(piece * third, 128))

    def see_all(b):
        def one(t, carry):
            see(b, t)
            return carry
        lax.fori_loop(0, 3, one, 0)

    see_all(me)
    aux_d2d.wait_recv()
    d2d_copy(buf.at[partner], CW, 0, 0).wait_recv()
    see_all(partner)

    def ring_arrival(way, d, item, piece, onward, to_x):
        b = 2 * from_at(way, d) + core
        ref = buf.at[b, piece]
        ring_copy(ref, way, d, item).wait_recv()
        if onward:
            ring_copy(ref, way, d + 1, item).start()
        if to_x:
            x_copy(ref, way, d).start()
        d2d_copy(ref, way, d, item).start()

    def aux_arrival(way, d, onward):
        b = 2 * from_at(way, d) + core
        ref = aux.at[b]
        ring_copy(ref, way, d, AUX).wait_recv()
        if onward:
            ring_copy(ref, way, d + 1, AUX).start()
        d2d_copy(ref, way, d, AUX).start()

    def x_arrival(way, d, onward):
        b = 2 * from_at(way, d) + core
        ref = buf.at[b, piece_tx]
        x_copy(ref, way, d).wait_recv()
        if onward:
            ring_copy(ref, way, d + 1, TX).start()
        d2d_copy(ref, way, d, TX).start()

    def d2d_arrival(way, d, item, piece):
        b = 2 * from_at(way, d) + 1 - core
        ref = aux.at[b] if item == AUX else buf.at[b, piece]
        d2d_copy(ref, way, d, item).wait_recv()

    def see_list(entries):
        for way, d, item, piece in entries:
            see(2 * from_at(way, d) + core, piece)
        for way, d, item, piece in entries:
            d2d_arrival(way, d, item, piece)
            see(2 * from_at(way, d) + 1 - core, piece)

    def turn(d, with_x, last):
        for way in (CW, CCW):
            aux_arrival(way, d, onward=not last or way == CW)
        ring_arrival(CW, d, 0, piece_x, onward=True, to_x=True)
        ring_arrival(CCW, d, 0, 1, onward=True, to_x=False)
        if with_x:
            x_arrival(CW, d - 1, False)
        for way in (CW, CCW):
            d2d_arrival(way, d, AUX, None)
        entries = [(CW, d, 0, piece_x), (CCW, d, 0, 1)]
        if with_x:
            entries.append((CW, d - 1, TX, piece_tx))
        see_list(entries)
        ring_arrival(CW, d, 1, 1, onward=not last, to_x=False)
        ring_arrival(CCW, d, 1, piece_x, onward=not last, to_x=True)
        if with_x:
            x_arrival(CCW, d - 1, False)
        entries = [(CW, d, 1, 1), (CCW, d, 1, piece_x)]
        if with_x:
            entries.append((CCW, d - 1, TX, piece_tx))
        see_list(entries)

    turn(1, False, far == 2)
    if far > 3:
        lax.fori_loop(2, far - 1, lambda d, c: (turn(d, True, False), c)[1], 0)
    if far > 2:
        turn(far - 1, True, True)
    x_arrival(CW, far - 1, True)
    aux_arrival(CW, far, False)
    ring_arrival(CW, far, 0, piece_x, False, False)
    ring_arrival(CCW, far, 0, 1, False, False)
    d2d_arrival(CW, far, AUX, None)
    see_list([(CW, far - 1, TX, piece_tx), (CW, far, 0, piece_x), (CCW, far, 0, 1)])
    x_arrival(CCW, far - 1, False)
    see_list([(CCW, far - 1, TX, piece_tx)])
    ring_arrival(CW, far, TX, piece_tx, False, False)
    see_list([(CW, far, TX, piece_tx)])

    lane = lax.broadcasted_iota(jnp.int32, (rows, 128), 1).astype(jnp.float32)
    for h in range(K // 128):
        cut = slice(h * 128, (h + 1) * 128)
        mine = jnp.where(lcol[...] == lane + float(h * 128), acc[:, cut], 0.0)
        wsrc[:, cut] = jnp.sum(mine, axis=0, keepdims=True)

    def within_copy(o, sender):
        return pltpu.make_async_remote_copy(
            src_ref=wsrc, dst_ref=wbuf.at[sender], send_sem=w_s.at[o], recv_sem=w_r.at[o],
            device_id=(layer, (me + o) % nb), device_id_type=MESH)

    def send_within(o, carry):
        within_copy(o, me).start()
        return carry

    lax.fori_loop(1, nb, send_within, 0)
    ones = jnp.ones((8, K), jnp.bfloat16)
    counts = lax.dot_general(ones, mem_acc[...].astype(jnp.bfloat16).T, (((1,), (0,)), ((), ())),
                             preferred_element_type=jnp.float32)[0:1, :]
    factor = 2.0 / counts
    acc[...] = 1.0 - acc[...] * factor

    def drain(d):
        for way in (CW, CCW):
            for item in (0, 1):
                ring_copy(buf.at[me, 0], way, d, item).wait_send()
                d2d_copy(buf.at[me, 0], way, d, item).wait_send()
            ring_copy(aux.at[me], way, d, AUX).wait_send()
            d2d_copy(aux.at[me], way, d, AUX).wait_send()
            d2d_copy(buf.at[me, 0], way, d, TX).wait_send()
            x_copy(buf.at[me, 0], way, d).wait_send()

    lax.fori_loop(1, far, lambda d, c: (drain(d), c)[1], 0)
    ring_copy(buf.at[me, 0], CW, far, 0).wait_send()
    ring_copy(buf.at[me, 0], CCW, far, 0).wait_send()
    ring_copy(buf.at[me, 0], CW, far, TX).wait_send()
    ring_copy(aux.at[me], CW, far, AUX).wait_send()
    d2d_copy(buf.at[me, 0], CW, far, 0).wait_send()
    d2d_copy(buf.at[me, 0], CCW, far, 0).wait_send()
    d2d_copy(buf.at[me, 0], CW, far, TX).wait_send()
    d2d_copy(aux.at[me], CW, far, AUX).wait_send()
    d2d_copy(aux.at[me], CW, 0, AUX).wait_send()
    d2d_copy(buf.at[me], CW, 0, 0).wait_send()

    def wait_within(o, total):
        sender = (me - o + nb) % nb
        copy = within_copy(o, sender)
        copy.wait_recv()
        copy.wait_send()
        return total + wbuf[sender]

    within = lax.fori_loop(1, nb, wait_within, wsrc[...])
    out_ref[...] = acc[...] + within / (counts * counts)


def solution(mesh):
    layers, nb = mesh.shape["layer"], mesh.shape["blk"]

    def shards(points, labels):
        rows, feat = points.shape
        third = rows // 3
        far = nb // 4
        sems = pltpu.SemaphoreType.DMA
        vmem = nb * rows * feat * 2 + 16 * 1024 * 1024
        return pl.pallas_call(
            functools.partial(kernel, layers, nb),
            out_shape=jax.ShapeDtypeStruct((rows, K), jnp.float32),
            in_specs=[pl.BlockSpec(memory_space=pl.ANY), pl.BlockSpec(memory_space=pltpu.VMEM)],
            out_specs=pl.BlockSpec(memory_space=pltpu.VMEM),
            scratch_shapes=[
                pltpu.VMEM((nb, 3, third, feat), jnp.bfloat16),
                pltpu.VMEM((nb, 1, 2 * rows), jnp.float32),
                pltpu.VMEM((rows, K), jnp.float32),
                pltpu.VMEM((K, third), jnp.float32),
                pltpu.VMEM((rows, 128), jnp.float32),
                pltpu.VMEM((rows, 128), jnp.float32),
                pltpu.VMEM((1, 2 * rows), jnp.float32),
                pltpu.VMEM((1, K), jnp.float32),
                pltpu.VMEM((nb, 1, K), jnp.float32),
                sems((3,)),
                sems((2, far + 1, 4)),
                sems((2, far + 1, 4)),
                sems((2, far + 1, 4)),
                sems((2, far + 1, 4)),
                sems((2, far + 1)),
                sems((2, far + 1)),
                sems((nb,)),
                sems((nb,)),
            ],
            compiler_params=pltpu.CompilerParams(
                collective_id=0, has_side_effects=True, vmem_limit_bytes=vmem),
        )(points, labels)

    return jax.shard_map(
        shards, mesh=mesh, in_specs=(P("blk", None), P("blk")), out_specs=P("blk", None), check_vma=False)
```

```python
import functools
import math

import jax
import jax.numpy as jnp
from jax import lax
from jax.experimental import pallas as pl
from jax.experimental.pallas import tpu as pltpu
from jax.sharding import PartitionSpec as P

K = 256
MESH = pl.DeviceIdType.MESH
NT = (((1,), (1,)), ((), ()))
CW, CCW = 0, 1
AUX, TX = 2, 3


def kernel(layers, nb, p_ref, lab_ref, out_ref, buf, aux, acc, mem_acc, rcol, lcol, own_aux, wsrc, wbuf, wmine, wpeer,
           local_sem, ring_s, ring_r, d2d_s, d2d_r, x_s, x_r, w_s, w_r):
    rows, feat = p_ref.shape
    third = rows // 3
    groups = nb // 2
    far = groups // 2
    layer = lax.axis_index("layer")
    me = lax.axis_index("blk")
    core = me % 2
    group = me // 2
    low, odd = group // 2, group % 2
    place = low + odd * (groups - 1 - 2 * low)

    def group_at(pos):
        pos = (pos + groups) % groups
        side = pos // far
        return 2 * (pos + side * (groups - 1 - 2 * pos)) + side

    other_layer = layer + 1 - 2 * (layer % 2)
    side = layer % 2
    partner = 2 * group + 1 - core
    nexts = (2 * group_at(place + 1) + core, 2 * group_at(place - 1) + core)
    piece_x, piece_tx = 2 * side, 2 - 2 * side

    def from_at(way, d):
        return group_at(place - d) if way == CW else group_at(place + d)

    def ring_copy(src, way, d, item, device=None):
        return pltpu.make_async_remote_copy(
            src_ref=src, dst_ref=src, send_sem=ring_s.at[way, d, item], recv_sem=ring_r.at[way, d, item],
            device_id=(layer, nexts[way]), device_id_type=MESH)

    def d2d_copy(src, way, d, item):
        return pltpu.make_async_remote_copy(
            src_ref=src, dst_ref=src, send_sem=d2d_s.at[way, d, item], recv_sem=d2d_r.at[way, d, item],
            device_id=(layer, partner), device_id_type=MESH)

    def x_copy(src, way, d):
        return pltpu.make_async_remote_copy(
            src_ref=src, dst_ref=src, send_sem=x_s.at[way, d], recv_sem=x_r.at[way, d],
            device_id=(other_layer, me), device_id_type=MESH)

    own_load = [pltpu.make_async_copy(p_ref.at[pl.ds(t * third, third)], buf.at[me, t], local_sem.at[t])
                for t in range(3)]
    for copy in own_load:
        copy.start()

    barrier = pltpu.get_barrier_semaphore()

    for place_of in ((layer, nexts[CW]), (layer, nexts[CCW]), (layer, partner), (other_layer, me)):
        pl.semaphore_signal(barrier, inc=1, device_id=place_of, device_id_type=MESH)
    for copy in own_load:
        copy.wait()

    pl.semaphore_wait(barrier, 4)
    ring_copy(buf.at[me, piece_x], CW, 1, 0).start()
    ring_copy(buf.at[me, 1], CCW, 1, 0).start()
    d2d_copy(buf.at[me], CW, 0, 0).start()

    scale = math.log2(math.e) / feat
    for t in range(3):
        part = slice(t * third, (t + 1) * third)
        x = buf[me, t].astype(jnp.float32)
        sq = jnp.sum(x * x, axis=1, keepdims=True) * scale
        wide = jnp.broadcast_to(sq, (third, 128))
        rcol[part, :] = wide
        own_aux[:, part] = wide.T[0:1, :]
    lab = lab_ref[...].reshape(1, rows).astype(jnp.float32)
    own_aux[:, rows:] = lab
    lcol[...] = jnp.broadcast_to(lab, (128, rows)).T
    acc[...] = jnp.zeros_like(acc)
    mem_acc[...] = jnp.zeros_like(mem_acc)

    def aux_send(way):
        return pltpu.make_async_remote_copy(
            src_ref=own_aux, dst_ref=aux.at[me], send_sem=ring_s.at[way, 1, AUX], recv_sem=ring_r.at[way, 1, AUX],
            device_id=(layer, nexts[way]), device_id_type=MESH)

    aux_d2d = pltpu.make_async_remote_copy(
        src_ref=own_aux, dst_ref=aux.at[me], send_sem=d2d_s.at[CW, 0, AUX], recv_sem=d2d_r.at[CW, 0, AUX],
        device_id=(layer, partner), device_id_type=MESH)

    for way in (CW, CCW):
        aux_send(way).start()
    ring_copy(buf.at[me, 1], CW, 1, 1).start()
    ring_copy(buf.at[me, piece_x], CCW, 1, 1).start()
    aux_d2d.start()

    ids = lax.broadcasted_iota(jnp.int32, (K, third), 0).astype(jnp.float32)
    own_copy = pltpu.make_async_copy(own_aux, aux.at[me], local_sem.at[0])
    own_copy.start()
    own_copy.wait()

    def visit(b, piece, offset, kind):
        cols = buf[b, piece]
        col_sq = aux[b, :, pl.ds(offset, third)]
        tags = aux[b, :, pl.ds(pl.multiple_of(rows + offset, 128), third)]
        member = (tags == ids).astype(jnp.float32)
        mem_acc[...] += member
        member = member.astype(jnp.bfloat16)
        for r in range(3):
            part = slice(r * third, (r + 1) * third)
            gram = lax.dot_general(buf[me, r], cols, NT, preferred_element_type=jnp.float32)
            row_sq = rcol[part, :]
            row_sq = jnp.concatenate([row_sq] * (third // 128), axis=1)
            kern = jnp.exp2(gram * (2.0 * scale) - (row_sq + col_sq)).astype(jnp.bfloat16)
            acc[kind, part, :] += lax.dot_general(kern, member, NT, preferred_element_type=jnp.float32)

    def see(b, piece):
        visit(b, piece, pl.multiple_of(piece * third, 128), piece)

    def see_all(b):
        def one(t, carry):
            see(b, t)
            return carry
        lax.fori_loop(0, 3, one, 0)

    see_all(me)
    aux_d2d.wait_recv()
    d2d_copy(buf.at[partner], CW, 0, 0).wait_recv()
    see_all(partner)

    def ring_arrival(way, d, item, piece, onward, to_x):
        b = 2 * from_at(way, d) + core
        ref = buf.at[b, piece]
        ring_copy(ref, way, d, item).wait_recv()
        if onward:
            ring_copy(ref, way, d + 1, item).start()
        if to_x:
            x_copy(ref, way, d).start()
        d2d_copy(ref, way, d, item).start()

    def aux_arrival(way, d, onward):
        b = 2 * from_at(way, d) + core
        ref = aux.at[b]
        ring_copy(ref, way, d, AUX).wait_recv()
        if onward:
            ring_copy(ref, way, d + 1, AUX).start()
        d2d_copy(ref, way, d, AUX).start()

    def x_arrival(way, d, onward):
        b = 2 * from_at(way, d) + core
        ref = buf.at[b, piece_tx]
        x_copy(ref, way, d).wait_recv()
        if onward:
            ring_copy(ref, way, d + 1, TX).start()
        d2d_copy(ref, way, d, TX).start()

    def d2d_arrival(way, d, item, piece):
        b = 2 * from_at(way, d) + 1 - core
        ref = aux.at[b] if item == AUX else buf.at[b, piece]
        d2d_copy(ref, way, d, item).wait_recv()

    def see_list(entries):
        for way, d, item, piece in entries:
            see(2 * from_at(way, d) + core, piece)
        for way, d, item, piece in entries:
            d2d_arrival(way, d, item, piece)
            see(2 * from_at(way, d) + 1 - core, piece)

    def turn(d, with_x, last):
        for way in (CW, CCW):
            aux_arrival(way, d, onward=not last or way == CW)
        ring_arrival(CW, d, 0, piece_x, onward=True, to_x=True)
        ring_arrival(CCW, d, 0, 1, onward=True, to_x=False)
        if with_x:
            x_arrival(CW, d - 1, False)
        for way in (CW, CCW):
            d2d_arrival(way, d, AUX, None)
        entries = [(CW, d, 0, piece_x), (CCW, d, 0, 1)]
        if with_x:
            entries.append((CW, d - 1, TX, piece_tx))
        see_list(entries)
        ring_arrival(CW, d, 1, 1, onward=not last, to_x=False)
        ring_arrival(CCW, d, 1, piece_x, onward=not last, to_x=True)
        if with_x:
            x_arrival(CCW, d - 1, False)
        entries = [(CW, d, 1, 1), (CCW, d, 1, piece_x)]
        if with_x:
            entries.append((CCW, d - 1, TX, piece_tx))
        see_list(entries)

    turn(1, False, far == 2)
    if far > 3:
        lax.fori_loop(2, far - 1, lambda d, c: (turn(d, True, False), c)[1], 0)
    if far > 2:
        turn(far - 1, True, True)
    x_arrival(CW, far - 1, True)
    aux_arrival(CW, far, False)
    ring_arrival(CW, far, 0, piece_x, False, False)
    ring_arrival(CCW, far, 0, 1, False, False)
    d2d_arrival(CW, far, AUX, None)
    see_list([(CW, far - 1, TX, piece_tx), (CW, far, 0, piece_x), (CCW, far, 0, 1)])
    lane = lax.broadcasted_iota(jnp.int32, (rows, 128), 1).astype(jnp.float32)
    for h in range(K // 128):
        cut = slice(h * 128, (h + 1) * 128)
        mine = jnp.where(lcol[...] == lane + float(h * 128), acc[piece_x, :, cut] + 0.5 * acc[1, :, cut], 0.0)
        wmine[:, cut] = jnp.sum(mine, axis=0, keepdims=True)

    peer_copy = pltpu.make_async_remote_copy(
        src_ref=wmine, dst_ref=wpeer, send_sem=w_s.at[0], recv_sem=w_r.at[0],
        device_id=(other_layer, me), device_id_type=MESH)
    peer_copy.start()
    x_arrival(CCW, far - 1, False)
    see_list([(CCW, far - 1, TX, piece_tx)])
    peer_copy.wait()
    wsrc[...] = wmine[...] + wpeer[...]

    def within_copy(o, sender):
        return pltpu.make_async_remote_copy(
            src_ref=wsrc, dst_ref=wbuf.at[sender], send_sem=w_s.at[o], recv_sem=w_r.at[o],
            device_id=(layer, (me + o) % nb), device_id_type=MESH)

    def send_within(o, carry):
        within_copy(o, me).start()
        return carry

    lax.fori_loop(1, nb, send_within, 0)
    ring_arrival(CW, far, TX, piece_tx, False, False)
    see_list([(CW, far, TX, piece_tx)])
    ones = jnp.ones((8, K), jnp.bfloat16)
    counts = lax.dot_general(ones, mem_acc[...].astype(jnp.bfloat16).T, (((1,), (0,)), ((), ())),
                             preferred_element_type=jnp.float32)[0:1, :]
    factor = 2.0 / counts

    def drain(d):
        for way in (CW, CCW):
            for item in (0, 1):
                ring_copy(buf.at[me, 0], way, d, item).wait_send()
                d2d_copy(buf.at[me, 0], way, d, item).wait_send()
            ring_copy(aux.at[me], way, d, AUX).wait_send()
            d2d_copy(aux.at[me], way, d, AUX).wait_send()
            d2d_copy(buf.at[me, 0], way, d, TX).wait_send()
            x_copy(buf.at[me, 0], way, d).wait_send()

    lax.fori_loop(1, far, lambda d, c: (drain(d), c)[1], 0)
    ring_copy(buf.at[me, 0], CW, far, 0).wait_send()
    ring_copy(buf.at[me, 0], CCW, far, 0).wait_send()
    ring_copy(buf.at[me, 0], CW, far, TX).wait_send()
    ring_copy(aux.at[me], CW, far, AUX).wait_send()
    d2d_copy(buf.at[me, 0], CW, far, 0).wait_send()
    d2d_copy(buf.at[me, 0], CCW, far, 0).wait_send()
    d2d_copy(buf.at[me, 0], CW, far, TX).wait_send()
    d2d_copy(aux.at[me], CW, far, AUX).wait_send()
    d2d_copy(aux.at[me], CW, 0, AUX).wait_send()
    d2d_copy(buf.at[me], CW, 0, 0).wait_send()

    def wait_within(o, total):
        sender = (me - o + nb) % nb
        copy = within_copy(o, sender)
        copy.wait_recv()
        copy.wait_send()
        return total + wbuf[sender]

    within = lax.fori_loop(1, nb, wait_within, wsrc[...])
    out_ref[...] = 1.0 + within / (counts * counts) - (acc[0] + acc[1] + acc[2]) * factor


def solution(mesh):
    layers, nb = mesh.shape["layer"], mesh.shape["blk"]

    def shards(points, labels):
        rows, feat = points.shape
        third = rows // 3
        far = nb // 4
        sems = pltpu.SemaphoreType.DMA
        vmem = nb * rows * feat * 2 + 16 * 1024 * 1024
        return pl.pallas_call(
            functools.partial(kernel, layers, nb),
            out_shape=jax.ShapeDtypeStruct((rows, K), jnp.float32),
            in_specs=[pl.BlockSpec(memory_space=pl.ANY), pl.BlockSpec(memory_space=pltpu.VMEM)],
            out_specs=pl.BlockSpec(memory_space=pltpu.VMEM),
            scratch_shapes=[
                pltpu.VMEM((nb, 3, third, feat), jnp.bfloat16),
                pltpu.VMEM((nb, 1, 2 * rows), jnp.float32),
                pltpu.VMEM((3, rows, K), jnp.float32),
                pltpu.VMEM((K, third), jnp.float32),
                pltpu.VMEM((rows, 128), jnp.float32),
                pltpu.VMEM((rows, 128), jnp.float32),
                pltpu.VMEM((1, 2 * rows), jnp.float32),
                pltpu.VMEM((1, K), jnp.float32),
                pltpu.VMEM((nb, 1, K), jnp.float32),
                pltpu.VMEM((1, K), jnp.float32),
                pltpu.VMEM((1, K), jnp.float32),
                sems((3,)),
                sems((2, far + 1, 4)),
                sems((2, far + 1, 4)),
                sems((2, far + 1, 4)),
                sems((2, far + 1, 4)),
                sems((2, far + 1)),
                sems((2, far + 1)),
                sems((nb,)),
                sems((nb,)),
            ],
            compiler_params=pltpu.CompilerParams(
                collective_id=0, has_side_effects=True, vmem_limit_bytes=vmem),
        )(points, labels)

    return jax.shard_map(
        shards, mesh=mesh, in_specs=(P("blk", None), P("blk")), out_specs=P("blk", None), check_vma=False)
```
